32 devices in a mesh: gy: 8 (over y, x, core), gz: 4 (over z).
Axes of the slice: x: 2, y: 2, z: 4, core: 2. Of those that a mesh axis runs over, the one named last changes fastest.
Arguments:
- observed: float32 [512, 128, 128], P(None, 'gy', 'gz'), may hold values from -6 to 6
- bregman: float32 [3, 512, 128, 128], P(None, None, 'gy', 'gz'), may hold values from -6 to 6
Outputs:
- solution: float32 [512, 128, 128], P(None, 'gy', 'gz')
- bregman_out: float32 [3, 512, 128, 128], P(None, None, 'gy', 'gz')
The draws below stay inside these ranges and needn't reach their ends.
All inputs are finite; a program needn't handle non-finite values.
Results may differ from the reference program's by a relative error of at most 0.0003.
Values sent between devices are 32-bit elements.
A program may use at most 128 MiB of HBM per device.

```python
import jax
import jax.numpy as jnp

NX = 512
ITERS = 3
NY = 128
NZ = 128


def block_levels(key, shape, shards, least, largest):
    def one(dim, parts):
        draws = jax.random.uniform(jax.random.fold_in(jax.random.fold_in(key, 6), dim), (parts,), jnp.float32, least / len(shards), largest / len(shards))
        return jnp.repeat(jnp.exp(draws), shape[dim] // parts).reshape((-1,) + (1,) * (len(shape) - dim - 1))

    level = one(*shards[0])
    for cut in shards[1:]:
        level = level * one(*cut)
    return level


def bell_draw(rng, extent, spread, reach, split=(), dtype=jnp.bfloat16):
    gain = block_levels(rng, extent, split, -0.22, 0.18) if split else 1.0
    drawn = jax.random.normal(rng, extent, jnp.float32) * spread * gain
    return jnp.minimum(jnp.maximum(drawn, -reach), reach).astype(dtype)


def setup_inputs(seed: int = 0) -> dict:
    key_list = jax.random.split(jax.random.key(seed), 3)
    observed = bell_draw(key_list[0], (NX, NY, NZ), 1.0, 6.0, ((1, 8), (2, 4)), jnp.float32)
    bregman = bell_draw(key_list[1], (3, NX, NY, NZ), 0.5, 6.0, ((2, 8), (3, 4)), jnp.float32)
    return {"observed": observed, "bregman": bregman}


fidelity = 1.0
penalty = 2.0
threshold = 0.5

def forward_cosine(values, axis):
    moved = jnp.moveaxis(values, axis, -1)
    length = moved.shape[-1]
    spectrum = jnp.fft.fft(moved, n=2 * length, axis=-1)[..., :length]
    wave = jnp.arange(length)
    twist = jnp.exp(-1j * jnp.pi * wave / (2 * length))
    factor = jnp.where(wave == 0, jnp.sqrt(1.0 / length), jnp.sqrt(2.0 / length))
    result = (jnp.real(spectrum * twist) * factor).astype(jnp.float32)
    return jnp.moveaxis(result, -1, axis)

def inverse_cosine(values, axis):
    moved = jnp.moveaxis(values, axis, -1)
    length = moved.shape[-1]
    wave = jnp.arange(length)
    twist = jnp.exp(1j * jnp.pi * wave / (2 * length))
    factor = jnp.where(wave == 0, jnp.sqrt(1.0 / length), jnp.sqrt(2.0 / length))
    weighted = moved * factor * twist
    padded = jnp.concatenate([weighted, jnp.zeros_like(weighted)], axis=-1)
    signal = jnp.fft.ifft(padded, axis=-1)[..., :length] * (2 * length)
    return jnp.moveaxis(jnp.real(signal).astype(jnp.float32), -1, axis)

def laplace_values(length):
    wave = jnp.arange(length).astype(jnp.float32)
    return 2.0 - 2.0 * jnp.cos(jnp.pi * wave / length)

def solve(source):
    spectra = forward_cosine(forward_cosine(forward_cosine(source, 0), 1), 2)
    divisor = fidelity + penalty * (laplace_values(source.shape[0])[:, None, None] + laplace_values(source.shape[1])[None, :, None] + laplace_values(source.shape[2])[None, None, :])
    spectra = spectra / divisor
    return inverse_cosine(inverse_cosine(inverse_cosine(spectra, 2), 1), 0)

def forward_step(volume, axis):
    moved = jnp.moveaxis(volume, axis, 0)
    result = jnp.concatenate([moved[1:] - moved[:-1], jnp.zeros_like(moved[:1])], axis=0)
    return jnp.moveaxis(result, 0, axis)

def gradients(volume):
    return jnp.stack([forward_step(volume, 0), forward_step(volume, 1), forward_step(volume, 2)])

def backward_step(component, axis):
    moved = jnp.moveaxis(component, axis, 0)
    masked = jnp.concatenate([moved[:-1], jnp.zeros_like(moved[:1])], axis=0)
    result = jnp.concatenate([jnp.zeros_like(masked[:1]), masked[:-1]], axis=0) - masked
    return jnp.moveaxis(result, 0, axis)

def adjoint(fluxes):
    result = backward_step(fluxes[0], 0)
    result = result + backward_step(fluxes[1], 1)
    return result + backward_step(fluxes[2], 2)

def shrink(values):
    return jnp.sign(values) * jnp.maximum(jnp.abs(values) - threshold, 0.0)

def reference(observed, bregman):
    shrunk = shrink(gradients(observed) + bregman)
    solution = observed
    for iteration in range(ITERS):
        source = fidelity * observed + penalty * adjoint(shrunk - bregman)
        solution = solve(source)
        slopes = gradients(solution)
        shrunk = shrink(slopes + bregman)
        bregman = bregman + slopes - shrunk
    return (solution, bregman)
```

```python
import functools

import jax
import jax.numpy as jnp
import numpy as np
from jax import lax
from jax.experimental import pallas as pl
from jax.experimental.pallas import tpu as pltpu
from jax.sharding import PartitionSpec as P

ITERS = 3
fidelity = 1.0
penalty = 2.0
threshold = 0.5
LANES = 128
OCTET = 8


def cosine_matrix(length):
    wave = np.arange(length)[:, None]
    sample = np.arange(length)[None, :]
    factor = np.where(wave == 0, np.sqrt(1.0 / length), np.sqrt(2.0 / length))
    return factor * np.cos(np.pi * ((2 * sample + 1) * wave % (4 * length)) / (2.0 * length))


def laplace_values(length):
    return 4.0 * np.sin(np.pi * np.arange(length) / (2.0 * length)) ** 2


def halves(matrix):
    matrix = matrix.astype(np.float32)
    high = matrix.astype(jnp.bfloat16)
    low = (matrix - high.astype(np.float32)).astype(jnp.bfloat16)
    return high, low


def split(values):
    high = values.astype(jnp.bfloat16)
    return high, (values - high.astype(jnp.float32)).astype(jnp.bfloat16)


def product(left, right, dims):
    dot = functools.partial(
        lax.dot_general, dimension_numbers=(dims, ((), ())), preferred_element_type=jnp.float32
    )
    return dot(left[0], right[0]) + (dot(left[0], right[1]) + dot(left[1], right[0]))


def swap_groups(arrays):
    arrays = list(arrays)
    lane = lax.broadcasted_iota(jnp.int32, arrays[0].shape, 1)
    for bit in (1, 2, 4):
        upper = (lane & bit) != 0
        for low in range(OCTET):
            if low & bit:
                continue
            first, second = arrays[low], arrays[low | bit]
            arrays[low] = jnp.where(upper, pltpu.roll(second, bit, 1), first)
            arrays[low | bit] = jnp.where(upper, second, pltpu.roll(first, LANES - bit, 1))
    return arrays


def clip(values):
    return jnp.minimum(jnp.maximum(values, -threshold), threshold)


def kernel(
    size_y, size_z,
    f_ref, b_in, xh, xl, yh, yl, th, tl, ex_ref, ey_ref,
    u_ref, b_ref,
    src, spec, front, depth, gain, tail, back, arrive, home, ends, gathered, chain, edge,
    next_y, last_y, next_z, last_z, pack_z, low_by, low_bz,
    fs, fr, bs, br, zs, zr, hs, hr,
):
    iy, iz = lax.axis_index("gy"), lax.axis_index("gz")
    cells_y, cells_z, extent = f_ref.shape
    octets = cells_z // OCTET
    part = extent // size_y
    groups = size_y // OCTET
    rows = cells_y * OCTET

    def at_y(d):
        return lax.rem(iy + d, size_y)

    def at_z(d):
        return lax.rem(iz + d, size_z)

    barrier = pltpu.get_barrier_semaphore()
    for d in range(1, size_y):
        pl.semaphore_signal(barrier, inc=1, device_id={"gy": at_y(d)}, device_id_type=pl.DeviceIdType.MESH)
    for d in range(1, size_z):
        pl.semaphore_signal(barrier, inc=1, device_id={"gz": at_z(d)}, device_id_type=pl.DeviceIdType.MESH)
    pl.semaphore_wait(barrier, size_y + size_z - 2)

    def remote(source, target, send, recv, device):
        return pltpu.make_async_remote_copy(
            src_ref=source, dst_ref=target, send_sem=send, recv_sem=recv,
            device_id=device, device_id_type=pl.DeviceIdType.MESH,
        )

    def halo_start(volume, slot):
        pack_z[slot, 0] = volume[:, 0, :]
        pack_z[slot, 1] = volume[:, cells_z - 1, :]
        copies = [
            remote(volume.at[0], next_y.at[slot], hs.at[slot, 0], hr.at[slot, 0], {"gy": at_y(size_y - 1)}),
            remote(volume.at[cells_y - 1], last_y.at[slot], hs.at[slot, 1], hr.at[slot, 1], {"gy": at_y(1)}),
            remote(pack_z.at[slot, 0], next_z.at[slot], hs.at[slot, 2], hr.at[slot, 2], {"gz": at_z(size_z - 1)}),
            remote(pack_z.at[slot, 1], last_z.at[slot], hs.at[slot, 3], hr.at[slot, 3], {"gz": at_z(1)}),
        ]
        for copy in copies:
            copy.start()
        return copies

    edge[...] = b_in[2, :, cells_z - 1, :]
    copies = halo_start(f_ref, 0)
    extra = [
        remote(b_in.at[1, cells_y - 1], low_by, hs.at[0, 4], hr.at[0, 4], {"gy": at_y(1)}),
        remote(edge, low_bz, hs.at[0, 5], hr.at[0, 5], {"gz": at_z(1)}),
    ]
    for copy in extra:
        copy.start()

    centre = (
        fidelity / penalty + 2.0
        + jnp.concatenate([ex_ref[pl.ds(pl.multiple_of(iy * part, part), part), :]] * groups, axis=1)
        + ey_ref[0:1, :]
    )

    def eliminate(first, final, keep):
        level = 1.0 / (centre - first)
        run = level
        corner = level
        if keep:
            gain[0] = level
            tail[0] = run

        def step(j, carry):
            level, run, corner = carry
            level = 1.0 / (centre - jnp.where(j == cells_z - 1, final, 0.0) - level)
            after = run * level
            corner = corner + run * after
            if keep:
                gain[j] = level
                tail[j] = after
            return level, after, corner

        return lax.fori_loop(1, cells_z, step, (level, run, corner))

    own_end, own_far, own_start = eliminate(
        jnp.where(iz == 0, 1.0, 0.0), jnp.where(iz == size_z - 1, 1.0, 0.0), True
    )
    mid_end, mid_far, mid_start = eliminate(0.0, 0.0, False)
    linked, _, _ = eliminate(1.0, 0.0, False)
    zero = jnp.zeros_like(centre)
    left_link = zero
    right_link = zero
    for q in range(size_z - 1):
        if q > 0:
            ratio = mid_far * linked / (1.0 - mid_start * linked)
            chain[q, 0] = mid_far + ratio * mid_start
            chain[q, 1] = ratio
            linked = mid_end + mid_far * ratio
        left_link = jnp.where(iz == q + 1, linked, left_link)
        right_link = jnp.where(size_z - 2 - iz == q, linked, right_link)
    one_l = 1.0 - own_start * left_link
    one_r = 1.0 - own_end * right_link
    cross_l = own_far * left_link
    cross_r = own_far * right_link
    scale = 1.0 / (one_l * one_r - cross_l * cross_r)
    home[0] = left_link
    home[1] = right_link
    home[2] = one_l * scale
    home[3] = one_r * scale
    home[4] = cross_l * scale
    home[5] = cross_r * scale
    home[6] = own_start
    home[7] = own_end
    home[8] = own_far

    for copy in copies + extra:
        copy.wait()

    lane_x = lax.broadcasted_iota(jnp.int32, (cells_z, extent), 1)
    row_z = lax.broadcasted_iota(jnp.int32, (cells_z, extent), 0)
    keep_x = lane_x < extent - 1
    keep_z = jnp.logical_or(row_z < cells_z - 1, iz < size_z - 1)

    def pointwise(volume, slopes_b, slot, first):
        def flux(slope, old):
            total = slope + old
            new = clip(total)
            return new, total - new - (old if first else new)

        new, lower_y = flux(volume[0] - last_y[slot], low_by[...])
        if not first:
            low_by[...] = new
        lower_y = jnp.where(iy > 0, lower_y, 0.0)
        new, lower_z = flux(pack_z[slot, 0] - last_z[slot], low_bz[...])
        if not first:
            low_bz[...] = new
        edge[...] = jnp.where(iz > 0, lower_z, 0.0)

        def plane(y, above, before, keep_y):
            value = volume[y]
            new, flux_x = flux(
                jnp.where(keep_x, pltpu.roll(value, extent - 1, 1) - value, 0.0), slopes_b[0, y]
            )
            b_ref[0, y] = slopes_b[0, y] if first else new
            flux_x = jnp.where(keep_x, flux_x, 0.0)
            new, flux_y = flux(jnp.where(keep_y, above - value, 0.0), slopes_b[1, y])
            b_ref[1, y] = slopes_b[1, y] if first else new
            flux_y = jnp.where(keep_y, flux_y, 0.0)
            beside = jnp.where(
                row_z < cells_z - 1, pltpu.roll(value, cells_z - 1, 0), next_z[slot, pl.ds(y, 1), :]
            )
            new, flux_z = flux(jnp.where(keep_z, beside - value, 0.0), slopes_b[2, y])
            b_ref[2, y] = slopes_b[2, y] if first else new
            flux_z = jnp.where(keep_z, flux_z, 0.0)
            under = jnp.where(row_z > 0, pltpu.roll(flux_z, 1, 0), edge[pl.ds(y, 1), :])
            src[y] = (
                (fidelity / penalty) * f_ref[y]
                + (pltpu.roll(flux_x, 1, 1) - flux_x)
                + (before - flux_y)
                + (under - flux_z)
            )
            return flux_y

        before = lax.fori_loop(
            0, cells_y - 1, lambda y, before: plane(y, volume[y + 1], before, True), lower_y
        )
        plane(cells_y - 1, next_y[slot], before, iy < size_y - 1)

    pointwise(f_ref, b_in, 0, True)

    def solve(slot):
        sent = []
        for o in range(octets):
            block = split(src[:, pl.ds(o * OCTET, OCTET), :].reshape(rows, extent))
            spec[o] = product((xh[...], xl[...]), block, ((1,), (1,)))
            for d in range(1, size_y):
                copy = remote(
                    spec.at[o, pl.ds(pl.multiple_of(at_y(d) * part, part), part)], front.at[o, iy],
                    fs.at[o, d], fr.at[o, d], {"gy": at_y(d)},
                )
                copy.start()
                sent.append(copy)
            front[o, iy] = spec[o, pl.ds(pl.multiple_of(iy * part, part), part), :]

        level = zero
        first = zero
        for o in range(octets):
            for copy in sent[o * (size_y - 1) : (o + 1) * (size_y - 1)]:
                copy.wait_recv()

            def regroup(r, _):
                at = pl.ds(pl.multiple_of(r * OCTET, OCTET), OCTET)
                for t in range(groups):
                    planes = swap_groups([front[o, t * OCTET + i, at, :] for i in range(OCTET)])
                    for i in range(OCTET):
                        depth[o * OCTET + i, at, pl.ds(t * LANES, LANES)] = planes[i]
                return 0

            lax.fori_loop(0, part // OCTET, regroup, 0, unroll=True)
            values = split(depth[pl.ds(o * OCTET, OCTET)].reshape(OCTET * part, size_y * cells_y))
            values = product(values, (yh[...], yl[...]), ((1,), (0,)))
            values = values.reshape(OCTET, part, size_y * cells_y)
            for i in range(OCTET):
                j = o * OCTET + i
                level = (values[i] + level) * gain[j]
                first = level if j == 0 else first + tail[j - 1] * level
                depth[j] = level
        ends[slot, 0] = first
        ends[slot, 1] = level
        gathered[slot, iz, 0] = first
        gathered[slot, iz, 1] = level

        around = []
        for d in range(1, size_z):
            copy = remote(
                ends.at[slot], gathered.at[slot, iz], zs.at[slot, d], zr.at[slot, d], {"gz": at_z(d)}
            )
            copy.start()
            around.append(copy)
        for copy in around:
            copy.wait_recv()
        left = zero
        right = zero
        for q in range(size_z - 1):
            here = gathered[slot, q, 1]
            there = gathered[slot, size_z - 1 - q, 0]
            if q > 0:
                here = here + chain[q, 0] * left + chain[q, 1] * gathered[slot, q, 0]
                there = there + chain[q, 0] * right + chain[q, 1] * gathered[slot, size_z - 1 - q, 1]
            left = jnp.where(q < iz, here, left)
            right = jnp.where(q < size_z - 1 - iz, there, right)
        bottom = first + home[6] * left + home[8] * right
        top = level + home[8] * left + home[7] * right
        from_left = left + home[0] * (home[3] * bottom + home[5] * top)
        value = right + home[1] * (home[2] * top + home[4] * bottom)

        returned = {}
        for o in reversed(range(octets)):
            for i in reversed(range(OCTET)):
                j = o * OCTET + i
                value = depth[j] + from_left * tail[j] + gain[j] * value
                depth[j] = value
            values = split(depth[pl.ds(o * OCTET, OCTET)].reshape(OCTET * part, size_y * cells_y))
            values = product(values, (th[...], tl[...]), ((1,), (0,)))
            depth[pl.ds(o * OCTET, OCTET)] = values.reshape(OCTET, part, size_y * cells_y)

            def ungroup(r, _):
                at = pl.ds(pl.multiple_of(r * OCTET, OCTET), OCTET)
                for t in range(groups):
                    planes = swap_groups(
                        [depth[o * OCTET + i, at, pl.ds(t * LANES, LANES)] for i in range(OCTET)]
                    )
                    for i in range(OCTET):
                        back[o, t * OCTET + i, at, :] = planes[i]
                return 0

            lax.fori_loop(0, part // OCTET, ungroup, 0, unroll=True)
            returned[o] = []
            for copy in sent[o * (size_y - 1) : (o + 1) * (size_y - 1)]:
                copy.wait_send()
            for d in range(1, size_y):
                copy = remote(
                    back.at[o, at_y(d)], arrive.at[o, pl.ds(pl.multiple_of(iy * part, part), part)],
                    bs.at[o, d], br.at[o, d], {"gy": at_y(d)},
                )
                copy.start()
                returned[o].append(copy)
            arrive[o, pl.ds(pl.multiple_of(iy * part, part), part), :] = back[o, iy]
        for o in reversed(range(octets)):
            for copy in returned[o]:
                copy.wait_recv()
            values = split(arrive[o].T)
            values = product(values, (xh[...], xl[...]), ((1,), (0,)))
            u_ref[:, pl.ds(o * OCTET, OCTET), :] = values.reshape(cells_y, OCTET, extent)
        for o in range(octets):
            for copy in returned[o]:
                copy.wait_send()
        for copy in around:
            copy.wait_send()

    def iteration(it, carry):
        solve(it)
        for copy in halo_start(u_ref, it + 1):
            copy.wait()
        pointwise(u_ref, b_ref, it + 1, False)
        return carry

    lax.fori_loop(0, ITERS, iteration, 0)


def per_device(size_y, size_z, observed, bregman):
    f = jnp.transpose(observed, (1, 2, 0))
    b = jnp.transpose(bregman, (0, 2, 3, 1))
    cells_y, cells_z, extent = f.shape
    full_y = cells_y * size_y
    part = extent // size_y
    octets = cells_z // OCTET
    groups = size_y // OCTET
    order = np.array(
        [
            (t * OCTET + i) * cells_y + y
            for t in range(groups)
            for y in range(cells_y)
            for i in range(OCTET)
        ]
    )
    matrix_y = cosine_matrix(full_y)[:, order]
    waves_x = np.broadcast_to(laplace_values(extent)[:, None], (extent, LANES))
    waves_y = np.broadcast_to(laplace_values(full_y)[None, :], (OCTET, full_y))
    constants = [
        *halves(cosine_matrix(extent)),
        *halves(matrix_y.T),
        *halves(matrix_y),
        waves_x.astype(np.float32),
        waves_y.astype(np.float32),
    ]
    slots = ITERS + 1
    real = lambda *shape: pltpu.VMEM(shape, jnp.float32)
    u, b = pl.pallas_call(
        functools.partial(kernel, size_y, size_z),
        out_shape=(
            jax.ShapeDtypeStruct(f.shape, jnp.float32),
            jax.ShapeDtypeStruct(b.shape, jnp.float32),
        ),
        in_specs=[pl.BlockSpec(memory_space=pltpu.VMEM)] * (2 + len(constants)),
        out_specs=(pl.BlockSpec(memory_space=pltpu.VMEM),) * 2,
        scratch_shapes=[
            real(cells_y, cells_z, extent),
            real(octets, extent, LANES),
            real(octets, size_y, part, LANES),
            real(cells_z, part, full_y),
            real(cells_z, part, full_y),
            real(cells_z, part, full_y),
            real(octets, size_y, part, LANES),
            real(octets, extent, LANES),
            real(9, part, full_y),
            real(ITERS, 2, part, full_y),
            real(ITERS, size_z, 2, part, full_y),
            real(size_z, 2, part, full_y),
            real(cells_y, extent),
            real(slots, cells_z, extent),
            real(slots, cells_z, extent),
            real(slots, cells_y, extent),
            real(slots, cells_y, extent),
            real(slots, 2, cells_y, extent),
            real(cells_z, extent),
            real(cells_y, extent),
            pltpu.SemaphoreType.DMA((octets, size_y)),
            pltpu.SemaphoreType.DMA((octets, size_y)),
            pltpu.SemaphoreType.DMA((octets, size_y)),
            pltpu.SemaphoreType.DMA((octets, size_y)),
            pltpu.SemaphoreType.DMA((ITERS, size_z)),
            pltpu.SemaphoreType.DMA((ITERS, size_z)),
            pltpu.SemaphoreType.DMA((slots, 6)),
            pltpu.SemaphoreType.DMA((slots, 6)),
        ],
        compiler_params=pltpu.CompilerParams(collective_id=0, has_side_effects=True),
    )(f, b, *[jnp.asarray(c) for c in constants])
    return jnp.transpose(u, (2, 0, 1)), jnp.transpose(b, (0, 3, 1, 2))


def solution(mesh):
    return jax.shard_map(
        functools.partial(per_device, mesh.shape["gy"], mesh.shape["gz"]),
        mesh=mesh,
        in_specs=(P(None, "gy", "gz"), P(None, None, "gy", "gz")),
        out_specs=(P(None, "gy", "gz"), P(None, None, "gy", "gz")),
        check_vma=False,
    )
```

```python
import functools

import jax
import jax.numpy as jnp
import numpy as np
from jax import lax
from jax.experimental import pallas as pl
from jax.experimental.pallas import tpu as pltpu
from jax.sharding import PartitionSpec as P

ITERS = 3
fidelity = 1.0
penalty = 2.0
threshold = 0.5
LANES = 128
OCTET = 8
HALVES = 2


def cosine_matrix(length):
    wave = np.arange(length)[:, None]
    sample = np.arange(length)[None, :]
    factor = np.where(wave == 0, np.sqrt(1.0 / length), np.sqrt(2.0 / length))
    return factor * np.cos(np.pi * ((2 * sample + 1) * wave % (4 * length)) / (2.0 * length))


def laplace_values(length):
    return 4.0 * np.sin(np.pi * np.arange(length) / (2.0 * length)) ** 2


def halves(matrix):
    matrix = matrix.astype(np.float32)
    high = matrix.astype(jnp.bfloat16)
    low = (matrix - high.astype(np.float32)).astype(jnp.bfloat16)
    return high, low


def split(values):
    high = values.astype(jnp.bfloat16)
    return high, (values - high.astype(jnp.float32)).astype(jnp.bfloat16)


def product(left, right, dims):
    dot = functools.partial(
        lax.dot_general, dimension_numbers=(dims, ((), ())), preferred_element_type=jnp.float32
    )
    return dot(left[0], right[0]) + (dot(left[0], right[1]) + dot(left[1], right[0]))


def swap_groups(arrays):
    arrays = list(arrays)
    lane = lax.broadcasted_iota(jnp.int32, arrays[0].shape, 1)
    for bit in (1, 2, 4):
        upper = (lane & bit) != 0
        for low in range(OCTET):
            if low & bit:
                continue
            first, second = arrays[low], arrays[low | bit]
            arrays[low] = jnp.where(upper, pltpu.roll(second, bit, 1), first)
            arrays[low | bit] = jnp.where(upper, second, pltpu.roll(first, LANES - bit, 1))
    return arrays


def clip(values):
    return jnp.minimum(jnp.maximum(values, -threshold), threshold)


def kernel(
    size_y, size_z,
    f_ref, b_in, xh, xl, yh, yl, th, tl, ex_ref, ey_ref,
    u_ref, b_ref,
    src, spec, front, depth, gain, tail, back, arrive, home, ends, gathered, chain, edge,
    next_y, last_y, next_z, last_z, pack_z, low_by, low_bz,
    fs, fr, bs, br, zs, zr, hs, hr, es, er,
):
    iy, iz = lax.axis_index("gy"), lax.axis_index("gz")
    cells_y, cells_z, extent = f_ref.shape
    octets = cells_z // OCTET
    part = extent // size_y
    piece = part // HALVES
    half = extent // HALVES
    groups = size_y // OCTET
    rows = cells_y * OCTET
    full_y = cells_y * size_y
    others_y = range(1, size_y)
    others_z = range(1, size_z)

    def at_y(d):
        return lax.rem(iy + d, size_y)

    def at_z(d):
        return lax.rem(iz + d, size_z)

    def octet(o):
        return pl.ds(o * OCTET, OCTET)

    barrier = pltpu.get_barrier_semaphore()
    for d in others_y:
        pl.semaphore_signal(barrier, inc=1, device_id={"gy": at_y(d)}, device_id_type=pl.DeviceIdType.MESH)
    for d in others_z:
        pl.semaphore_signal(barrier, inc=1, device_id={"gz": at_z(d)}, device_id_type=pl.DeviceIdType.MESH)
    pl.semaphore_wait(barrier, size_y + size_z - 2)

    def remote(source, target, send, recv, device):
        return pltpu.make_async_remote_copy(
            src_ref=source, dst_ref=target, send_sem=send, recv_sem=recv,
            device_id=device, device_id_type=pl.DeviceIdType.MESH,
        )

    def band(h, owner):
        return pl.ds(pl.multiple_of(h * half + owner * piece, piece), piece)

    def inner(h):
        return pl.ds(h * piece, piece)

    def forth(h, o, d):
        return remote(
            spec.at[o, band(h, at_y(d))], front.at[o, iy, inner(h)],
            fs.at[h, o, d], fr.at[h, o, d], {"gy": at_y(d)},
        )

    def home_copy(h, o, d):
        return remote(
            back.at[h, o, at_y(d)], arrive.at[o, band(h, iy)],
            bs.at[h, o, d], br.at[h, o, d], {"gy": at_y(d)},
        )

    def around(slot, h, d):
        return remote(
            ends.at[slot, h], gathered.at[slot, iz, h],
            zs.at[slot, h, d], zr.at[slot, h, d], {"gz": at_z(d)},
        )

    def halo_y(volume, slot, o):
        return [
            remote(
                volume.at[0, octet(o)], next_y.at[slot, octet(o)],
                hs.at[slot, 0, o], hr.at[slot, 0, o], {"gy": at_y(size_y - 1)},
            ),
            remote(
                volume.at[cells_y - 1, octet(o)], last_y.at[slot, octet(o)],
                hs.at[slot, 1, o], hr.at[slot, 1, o], {"gy": at_y(1)},
            ),
        ]

    def halo_next_z(slot):
        return remote(
            pack_z.at[slot, 0], next_z.at[slot], es.at[slot, 0], er.at[slot, 0],
            {"gz": at_z(size_z - 1)},
        )

    def halo_last_z(slot):
        return remote(
            pack_z.at[slot, 1], last_z.at[slot], es.at[slot, 1], er.at[slot, 1], {"gz": at_z(1)}
        )

    def halo_start(volume, slot, o):
        if o == 0:
            pack_z[slot, 0] = volume[:, 0, :]
            halo_next_z(slot).start()
        if o == octets - 1:
            pack_z[slot, 1] = volume[:, cells_z - 1, :]
            halo_last_z(slot).start()
        for copy in halo_y(volume, slot, o):
            copy.start()

    edge[...] = b_in[2, :, cells_z - 1, :]
    extra = [
        remote(b_in.at[1, cells_y - 1], low_by, es.at[0, 2], er.at[0, 2], {"gy": at_y(1)}),
        remote(edge, low_bz, es.at[0, 3], er.at[0, 3], {"gz": at_z(1)}),
    ]
    for copy in extra:
        copy.start()
    for o in range(octets):
        halo_start(f_ref, 0, o)

    waves = jnp.concatenate([ex_ref[band(h, iy), :] for h in range(HALVES)], axis=0)
    centre = fidelity / penalty + 2.0 + jnp.concatenate([waves] * groups, axis=1) + ey_ref[0:1, :]

    def eliminate(first, final, keep):
        level = 1.0 / (centre - first)
        run = level
        corner = level
        if keep:
            gain[0] = level
            tail[0] = run

        def step(j, carry):
            level, run, corner = carry
            level = 1.0 / (centre - jnp.where(j == cells_z - 1, final, 0.0) - level)
            after = run * level
            corner = corner + run * after
            if keep:
                gain[j] = level
                tail[j] = after
            return level, after, corner

        return lax.fori_loop(1, cells_z, step, (level, run, corner))

    def coefficients():
        own_end, own_far, own_start = eliminate(
            jnp.where(iz == 0, 1.0, 0.0), jnp.where(iz == size_z - 1, 1.0, 0.0), True
        )
        mid_end, mid_far, mid_start = eliminate(0.0, 0.0, False)
        linked, _, _ = eliminate(1.0, 0.0, False)
        left_link = jnp.zeros_like(centre)
        right_link = jnp.zeros_like(centre)
        for q in range(size_z - 1):
            if q > 0:
                ratio = mid_far * linked / (1.0 - mid_start * linked)
                chain[q, 0] = mid_far + ratio * mid_start
                chain[q, 1] = ratio
                linked = mid_end + mid_far * ratio
            left_link = jnp.where(iz == q + 1, linked, left_link)
            right_link = jnp.where(size_z - 2 - iz == q, linked, right_link)
        one_l = 1.0 - own_start * left_link
        one_r = 1.0 - own_end * right_link
        cross_l = own_far * left_link
        cross_r = own_far * right_link
        scale = 1.0 / (one_l * one_r - cross_l * cross_r)
        home[0] = left_link
        home[1] = right_link
        home[2] = one_l * scale
        home[3] = one_r * scale
        home[4] = cross_l * scale
        home[5] = cross_r * scale
        home[6] = own_start
        home[7] = own_end
        home[8] = own_far

    row = lax.broadcasted_iota(jnp.int32, (OCTET, extent), 0)
    keep_x = lax.broadcasted_iota(jnp.int32, (OCTET, extent), 1) < extent - 1

    def pointwise(volume, old, slot, first, o):
        at = octet(o)
        final = o == octets - 1

        def flux(slope, was):
            total = slope + was
            new = clip(total)
            return new, total - new - (was if first else new)

        if o == 0:
            if first:
                for copy in extra:
                    copy.wait()
            halo_last_z(slot).wait()
            new, lower_z = flux(pack_z[slot, 0] - last_z[slot], low_bz[...])
            if not first:
                low_bz[...] = new
            edge[...] = jnp.where(iz > 0, lower_z, 0.0)
        if final:
            halo_next_z(slot).wait()

        def plane(y, above, before, keep_y):
            value = volume[y, at, :]
            new, flux_x = flux(
                jnp.where(keep_x, pltpu.roll(value, extent - 1, 1) - value, 0.0), old[0, y, at, :]
            )
            b_ref[0, y, at, :] = old[0, y, at, :] if first else new
            flux_x = jnp.where(keep_x, flux_x, 0.0)
            new, flux_y = flux(jnp.where(keep_y, above - value, 0.0), old[1, y, at, :])
            b_ref[1, y, at, :] = old[1, y, at, :] if first else new
            flux_y = jnp.where(keep_y, flux_y, 0.0)
            if final:
                beyond = next_z[slot, pl.ds(y, 1), :]
                keep_z = jnp.logical_or(row < OCTET - 1, iz < size_z - 1)
            else:
                beyond = volume[y, pl.ds((o + 1) * OCTET, 1), :]
                keep_z = row < OCTET
            beside = jnp.where(row < OCTET - 1, pltpu.roll(value, OCTET - 1, 0), beyond)
            new, flux_z = flux(jnp.where(keep_z, beside - value, 0.0), old[2, y, at, :])
            b_ref[2, y, at, :] = old[2, y, at, :] if first else new
            flux_z = jnp.where(keep_z, flux_z, 0.0)
            under = pltpu.roll(flux_z, 1, 0)
            src[o, y] = (
                (fidelity / penalty) * f_ref[y, at, :]
                + (pltpu.roll(flux_x, 1, 1) - flux_x)
                + (before - flux_y)
                + (jnp.where(row > 0, under, edge[pl.ds(y, 1), :]) - flux_z)
            )
            edge[pl.ds(y, 1), :] = under[0:1, :]
            return flux_y

        _, bottom = flux(volume[1, at, :] - volume[0, at, :], old[1, 0, at, :])
        before = lax.fori_loop(
            1, cells_y - 1, lambda y, before: plane(y, volume[y + 1, at, :], before, True), bottom
        )
        for copy in halo_y(volume, slot, o):
            copy.wait()
        new, lower_y = flux(volume[0, at, :] - last_y[slot, at, :], low_by[at, :])
        if not first:
            low_by[at, :] = new
        plane(0, volume[1, at, :], jnp.where(iy > 0, lower_y, 0.0), True)
        plane(cells_y - 1, next_y[slot, at, :], before, iy < size_y - 1)

    def send_octet(o):
        block = split(src[o].reshape(rows, extent))
        spec[o] = product((xh[...], xl[...]), block, ((1,), (1,)))
        for d in others_y:
            forth(0, o, d).start()
        for h in range(HALVES):
            front[o, iy, inner(h), :] = spec[o, band(h, iy), :]

    def send_rest():
        for h in range(1, HALVES):
            for o in range(octets):
                for d in others_y:
                    forth(h, o, d).start()

    def forward(slot, h):
        level = jnp.zeros((piece, full_y), jnp.float32)
        first = level
        for o in range(octets):
            for d in others_y:
                forth(h, o, d).wait_recv()
            for r in range(piece // OCTET):
                at = pl.ds(h * piece + r * OCTET, OCTET)
                for t in range(groups):
                    planes = swap_groups([front[o, t * OCTET + i, at, :] for i in range(OCTET)])
                    for i in range(OCTET):
                        depth[h, o * OCTET + i, pl.ds(r * OCTET, OCTET), pl.ds(t * LANES, LANES)] = planes[i]
            values = split(depth[h, octet(o)].reshape(OCTET * piece, full_y))
            values = product(values, (yh[...], yl[...]), ((1,), (0,)))
            values = values.reshape(OCTET, piece, full_y)
            for i in range(OCTET):
                j = o * OCTET + i
                level = (values[i] + level) * gain[j, inner(h), :]
                first = level if j == 0 else first + tail[j - 1, inner(h), :] * level
                depth[h, j] = level
        ends[slot, h, 0] = first
        ends[slot, h, 1] = level
        gathered[slot, iz, h, 0] = first
        gathered[slot, iz, h, 1] = level
        for d in others_z:
            around(slot, h, d).start()

    def backward(slot, h):
        for d in others_z:
            around(slot, h, d).wait_recv()
        left = jnp.zeros((piece, full_y), jnp.float32)
        right = left
        for q in range(size_z - 1):
            mirror = size_z - 1 - q
            here = gathered[slot, q, h, 1]
            there = gathered[slot, mirror, h, 0]
            if q > 0:
                near, far = chain[q, 0, inner(h), :], chain[q, 1, inner(h), :]
                here = here + near * left + far * gathered[slot, q, h, 0]
                there = there + near * right + far * gathered[slot, mirror, h, 1]
            left = jnp.where(q < iz, here, left)
            right = jnp.where(q < size_z - 1 - iz, there, right)
        link = [home[i, inner(h), :] for i in range(9)]
        bottom = ends[slot, h, 0] + link[6] * left + link[8] * right
        top = ends[slot, h, 1] + link[8] * left + link[7] * right
        from_left = left + link[0] * (link[3] * bottom + link[5] * top)
        value = right + link[1] * (link[2] * top + link[4] * bottom)
        for o in reversed(range(octets)):
            for i in reversed(range(OCTET)):
                j = o * OCTET + i
                value = (
                    depth[h, j] + from_left * tail[j, inner(h), :] + gain[j, inner(h), :] * value
                )
                depth[h, j] = value
            values = split(depth[h, octet(o)].reshape(OCTET * piece, full_y))
            values = product(values, (th[...], tl[...]), ((1,), (0,)))
            depth[h, octet(o)] = values.reshape(OCTET, piece, full_y)
            for r in range(piece // OCTET):
                at = pl.ds(r * OCTET, OCTET)
                for t in range(groups):
                    planes = swap_groups(
                        [depth[h, o * OCTET + i, at, pl.ds(t * LANES, LANES)] for i in range(OCTET)]
                    )
                    for i in range(OCTET):
                        back[h, o, t * OCTET + i, at, :] = planes[i]
            for d in others_y:
                home_copy(h, o, d).start()
            arrive[o, band(h, iy), :] = back[h, o, iy]

    def assemble(slot, h):
        at = pl.ds(h * half, half)
        for o in reversed(range(octets)):
            for d in others_y:
                home_copy(h, o, d).wait_recv()
            values = product(split(arrive[o, at, :].T), (xh[at, :], xl[at, :]), ((1,), (0,)))
            values = values.reshape(cells_y, OCTET, extent)
            if h > 0:
                values = values + u_ref[:, octet(o), :]
            u_ref[:, octet(o), :] = values
            if h == HALVES - 1:
                halo_start(u_ref, slot + 1, o)

    coefficients()
    for o in range(octets):
        pointwise(f_ref, b_in, 0, True, o)
        send_octet(o)
    send_rest()

    def iteration(slot, carry):
        for h in range(HALVES):
            forward(slot, h)
        for h in range(HALVES):
            backward(slot, h)
        for h in range(HALVES):
            for o in range(octets):
                for d in others_y:
                    forth(h, o, d).wait_send()
        for h in range(HALVES):
            assemble(slot, h)
        for h in range(HALVES):
            for o in range(octets):
                for d in others_y:
                    home_copy(h, o, d).wait_send()
            for d in others_z:
                around(slot, h, d).wait_send()
        for o in range(octets):
            pointwise(u_ref, b_ref, slot + 1, False, o)

            @pl.when(slot < ITERS - 1)
            def _():
                send_octet(o)

        @pl.when(slot < ITERS - 1)
        def _():
            send_rest()

        return carry

    lax.fori_loop(0, ITERS, iteration, 0)


def per_device(size_y, size_z, observed, bregman):
    f = jnp.transpose(observed, (1, 2, 0))
    b = jnp.transpose(bregman, (0, 2, 3, 1))
    cells_y, cells_z, extent = f.shape
    full_y = cells_y * size_y
    part = extent // size_y
    octets = cells_z // OCTET
    groups = size_y // OCTET
    order = np.array(
        [
            (t * OCTET + i) * cells_y + y
            for t in range(groups)
            for y in range(cells_y)
            for i in range(OCTET)
        ]
    )
    matrix_y = cosine_matrix(full_y)[:, order]
    waves_x = np.broadcast_to(laplace_values(extent)[:, None], (extent, LANES))
    waves_y = np.broadcast_to(laplace_values(full_y)[None, :], (OCTET, full_y))
    constants = [
        *halves(cosine_matrix(extent)),
        *halves(matrix_y.T),
        *halves(matrix_y),
        waves_x.astype(np.float32),
        waves_y.astype(np.float32),
    ]
    slots = ITERS + 1
    piece = part // HALVES
    flags = pltpu.SemaphoreType.DMA
    real = lambda *shape: pltpu.VMEM(shape, jnp.float32)
    u, b = pl.pallas_call(
        functools.partial(kernel, size_y, size_z),
        out_shape=(
            jax.ShapeDtypeStruct(f.shape, jnp.float32),
            jax.ShapeDtypeStruct(b.shape, jnp.float32),
        ),
        in_specs=[pl.BlockSpec(memory_space=pltpu.VMEM)] * (2 + len(constants)),
        out_specs=(pl.BlockSpec(memory_space=pltpu.VMEM),) * 2,
        scratch_shapes=[
            real(octets, cells_y, OCTET, extent),
            real(octets, extent, LANES),
            real(octets, size_y, part, LANES),
            real(HALVES, cells_z, piece, full_y),
            real(cells_z, part, full_y),
            real(cells_z, part, full_y),
            real(HALVES, octets, size_y, piece, LANES),
            real(octets, extent, LANES),
            real(9, part, full_y),
            real(ITERS, HALVES, 2, piece, full_y),
            real(ITERS, size_z, HALVES, 2, piece, full_y),
            real(size_z, 2, part, full_y),
            real(cells_y, extent),
            real(slots, cells_z, extent),
            real(slots, cells_z, extent),
            real(slots, cells_y, extent),
            real(slots, cells_y, extent),
            real(slots, 2, cells_y, extent),
            real(cells_z, extent),
            real(cells_y, extent),
            flags((HALVES, octets, size_y)),
            flags((HALVES, octets, size_y)),
            flags((HALVES, octets, size_y)),
            flags((HALVES, octets, size_y)),
            flags((ITERS, HALVES, size_z)),
            flags((ITERS, HALVES, size_z)),
            flags((slots, 2, octets)),
            flags((slots, 2, octets)),
            flags((slots, 4)),
            flags((slots, 4)),
        ],
        compiler_params=pltpu.CompilerParams(collective_id=0, has_side_effects=True),
    )(f, b, *[jnp.asarray(c) for c in constants])
    return jnp.transpose(u, (2, 0, 1)), jnp.transpose(b, (0, 3, 1, 2))


def solution(mesh):
    return jax.shard_map(
        functools.partial(per_device, mesh.shape["gy"], mesh.shape["gz"]),
        mesh=mesh,
        in_specs=(P(None, "gy", "gz"), P(None, None, "gy", "gz")),
        out_specs=(P(None, "gy", "gz"), P(None, None, "gy", "gz")),
        check_vma=False,
    )
```

```python
import functools

import jax
import jax.numpy as jnp
import numpy as np
from jax import lax
from jax.experimental import pallas as pl
from jax.experimental.pallas import tpu as pltpu
from jax.sharding import PartitionSpec as P

ITERS = 3
fidelity = 1.0
penalty = 2.0
threshold = 0.5
LANES = 128
OCTET = 8
HALVES = 2


def cosine_matrix(length):
    wave = np.arange(length)[:, None]
    sample = np.arange(length)[None, :]
    factor = np.where(wave == 0, np.sqrt(1.0 / length), np.sqrt(2.0 / length))
    return factor * np.cos(np.pi * ((2 * sample + 1) * wave % (4 * length)) / (2.0 * length))


def laplace_values(length):
    return 4.0 * np.sin(np.pi * np.arange(length) / (2.0 * length)) ** 2


def halves(matrix):
    matrix = matrix.astype(np.float32)
    high = matrix.astype(jnp.bfloat16)
    low = (matrix - high.astype(np.float32)).astype(jnp.bfloat16)
    return high, low


def split(values):
    high = values.astype(jnp.bfloat16)
    return high, (values - high.astype(jnp.float32)).astype(jnp.bfloat16)


def product(left, right, dims):
    dot = functools.partial(
        lax.dot_general, dimension_numbers=(dims, ((), ())), preferred_element_type=jnp.float32
    )
    return dot(left[0], right[0]) + (dot(left[0], right[1]) + dot(left[1], right[0]))


def swap_groups(arrays):
    arrays = list(arrays)
    lane = lax.broadcasted_iota(jnp.int32, arrays[0].shape, 1)
    for bit in (1, 2, 4):
        upper = (lane & bit) != 0
        for low in range(OCTET):
            if low & bit:
                continue
            first, second = arrays[low], arrays[low | bit]
            arrays[low] = jnp.where(upper, pltpu.roll(second, bit, 1), first)
            arrays[low | bit] = jnp.where(upper, second, pltpu.roll(first, LANES - bit, 1))
    return arrays


def clip(values):
    return jnp.minimum(jnp.maximum(values, -threshold), threshold)


def kernel(
    size_y, size_z,
    f_ref, b_in, xh, xl, yh, yl, th, tl, ex_ref, ey_ref,
    u_ref, b_ref,
    src, spec, front, depth, gain, tail, back, arrive, home, ends, gathered, chain, edge, border,
    next_y, last_y, next_z, last_z, pack_z, low_by, low_bz,
    fs, fr, bs, br, zs, zr, hs, hr, es, er,
):
    iy, iz = lax.axis_index("gy"), lax.axis_index("gz")
    cells_y, cells_z, extent = f_ref.shape
    octets = cells_z // OCTET
    part = extent // size_y
    piece = part // HALVES
    half = extent // HALVES
    groups = size_y // OCTET
    rows = cells_y * OCTET
    full_y = cells_y * size_y
    others_y = range(1, size_y)
    others_z = range(1, size_z)

    def at_y(d):
        return lax.rem(iy + d, size_y)

    def at_z(d):
        return lax.rem(iz + d, size_z)

    def octet(o):
        return pl.ds(o * OCTET, OCTET)

    barrier = pltpu.get_barrier_semaphore()
    for d in others_y:
        pl.semaphore_signal(barrier, inc=1, device_id={"gy": at_y(d)}, device_id_type=pl.DeviceIdType.MESH)
    for d in others_z:
        pl.semaphore_signal(barrier, inc=1, device_id={"gz": at_z(d)}, device_id_type=pl.DeviceIdType.MESH)
    pl.semaphore_wait(barrier, size_y + size_z - 2)

    def remote(source, target, send, recv, device):
        return pltpu.make_async_remote_copy(
            src_ref=source, dst_ref=target, send_sem=send, recv_sem=recv,
            device_id=device, device_id_type=pl.DeviceIdType.MESH,
        )

    def band(h, owner):
        return pl.ds(pl.multiple_of(h * half + owner * piece, piece), piece)

    def inner(h):
        return pl.ds(h * piece, piece)

    def forth(h, o, d):
        return remote(
            spec.at[o, band(h, at_y(d))], front.at[o, iy, inner(h)],
            fs.at[h, o, d], fr.at[h, o, d], {"gy": at_y(d)},
        )

    def home_copy(h, o, d):
        return remote(
            back.at[h, o, at_y(d)], arrive.at[o, band(h, iy)],
            bs.at[h, o, d], br.at[h, o, d], {"gy": at_y(d)},
        )

    def around(slot, h, d):
        return remote(
            ends.at[slot, h], gathered.at[slot, iz, h],
            zs.at[slot, h, d], zr.at[slot, h, d], {"gz": at_z(d)},
        )

    def halo_y(volume, slot, o):
        return [
            remote(
                volume.at[0, octet(o)], next_y.at[slot, octet(o)],
                hs.at[slot, 0, o], hr.at[slot, 0, o], {"gy": at_y(size_y - 1)},
            ),
            remote(
                volume.at[cells_y - 1, octet(o)], last_y.at[slot, octet(o)],
                hs.at[slot, 1, o], hr.at[slot, 1, o], {"gy": at_y(1)},
            ),
        ]

    def halo_next_z(slot):
        return remote(
            pack_z.at[slot, 0], next_z.at[slot], es.at[slot, 0], er.at[slot, 0],
            {"gz": at_z(size_z - 1)},
        )

    def halo_last_z(slot):
        return remote(
            pack_z.at[slot, 1], last_z.at[slot], es.at[slot, 1], er.at[slot, 1], {"gz": at_z(1)}
        )

    def halo_start(volume, slot, o):
        if o == 0:
            pack_z[slot, 0] = volume[:, 0, :]
            halo_next_z(slot).start()
        if o == octets - 1:
            pack_z[slot, 1] = volume[:, cells_z - 1, :]
            halo_last_z(slot).start()
        for copy in halo_y(volume, slot, o):
            copy.start()

    edge[...] = b_in[2, :, cells_z - 1, :]
    extra = [
        remote(b_in.at[1, cells_y - 1], low_by, es.at[0, 2], er.at[0, 2], {"gy": at_y(1)}),
        remote(edge, low_bz, es.at[0, 3], er.at[0, 3], {"gz": at_z(1)}),
    ]
    for copy in extra:
        copy.start()
    for o in range(octets):
        halo_start(f_ref, 0, o)

    waves = jnp.concatenate([ex_ref[band(h, iy), :] for h in range(HALVES)], axis=0)
    centre = fidelity / penalty + 2.0 + jnp.concatenate([waves] * groups, axis=1) + ey_ref[0:1, :]

    def eliminate(first, final, keep):
        level = 1.0 / (centre - first)
        run = level
        corner = level
        if keep:
            gain[0] = level
            tail[0] = run

        def step(j, carry):
            level, run, corner = carry
            level = 1.0 / (centre - jnp.where(j == cells_z - 1, final, 0.0) - level)
            after = run * level
            corner = corner + run * after
            if keep:
                gain[j] = level
                tail[j] = after
            return level, after, corner

        return lax.fori_loop(1, cells_z, step, (level, run, corner))

    def coefficients():
        own_end, own_far, own_start = eliminate(
            jnp.where(iz == 0, 1.0, 0.0), jnp.where(iz == size_z - 1, 1.0, 0.0), True
        )
        mid_end, mid_far, mid_start = eliminate(0.0, 0.0, False)
        linked, _, _ = eliminate(1.0, 0.0, False)
        left_link = jnp.zeros_like(centre)
        right_link = jnp.zeros_like(centre)
        for q in range(size_z - 1):
            if q > 0:
                ratio = mid_far * linked / (1.0 - mid_start * linked)
                chain[q, 0] = mid_far + ratio * mid_start
                chain[q, 1] = ratio
                linked = mid_end + mid_far * ratio
            left_link = jnp.where(iz == q + 1, linked, left_link)
            right_link = jnp.where(size_z - 2 - iz == q, linked, right_link)
        one_l = 1.0 - own_start * left_link
        one_r = 1.0 - own_end * right_link
        cross_l = own_far * left_link
        cross_r = own_far * right_link
        scale = 1.0 / (one_l * one_r - cross_l * cross_r)
        home[0] = left_link
        home[1] = right_link
        home[2] = one_l * scale
        home[3] = one_r * scale
        home[4] = cross_l * scale
        home[5] = cross_r * scale
        home[6] = own_start
        home[7] = own_end
        home[8] = own_far

    row = lax.broadcasted_iota(jnp.int32, (OCTET, extent), 0)
    keep_x = lax.broadcasted_iota(jnp.int32, (OCTET, extent), 1) < extent - 1

    def pointwise(volume, old, slot, first, o):
        at = octet(o)
        final = o == octets - 1

        def flux(slope, was):
            total = slope + was
            new = clip(total)
            return new, total - new - (was if first else new)

        if o == 0:
            if first:
                for copy in extra:
                    copy.wait()
            halo_last_z(slot).wait()
            new, lower_z = flux(pack_z[slot, 0] - last_z[slot], low_bz[...])
            if not first:
                low_bz[...] = new
            lower_z = jnp.where(iz > 0, lower_z, 0.0)
            for y in range(cells_y):
                border[y, 0:1, :] = lower_z[y : y + 1, :]
        if final:
            halo_next_z(slot).wait()

        def plane(y, above, before, keep_y):
            value = volume[y, at, :]
            new, flux_x = flux(
                jnp.where(keep_x, pltpu.roll(value, extent - 1, 1) - value, 0.0), old[0, y, at, :]
            )
            b_ref[0, y, at, :] = old[0, y, at, :] if first else new
            flux_x = jnp.where(keep_x, flux_x, 0.0)
            new, flux_y = flux(jnp.where(keep_y, above - value, 0.0), old[1, y, at, :])
            b_ref[1, y, at, :] = old[1, y, at, :] if first else new
            flux_y = jnp.where(keep_y, flux_y, 0.0)
            if final:
                beyond = next_z[slot, pl.ds(y, 1), :]
                keep_z = jnp.logical_or(row < OCTET - 1, iz < size_z - 1)
            else:
                beyond = volume[y, pl.ds((o + 1) * OCTET, 1), :]
                keep_z = row < OCTET
            beside = jnp.where(row < OCTET - 1, pltpu.roll(value, OCTET - 1, 0), beyond)
            new, flux_z = flux(jnp.where(keep_z, beside - value, 0.0), old[2, y, at, :])
            b_ref[2, y, at, :] = old[2, y, at, :] if first else new
            flux_z = jnp.where(keep_z, flux_z, 0.0)
            under = pltpu.roll(flux_z, 1, 0)
            src[o, y] = (
                (fidelity / penalty) * f_ref[y, at, :]
                + (pltpu.roll(flux_x, 1, 1) - flux_x)
                + (before - flux_y)
                + (jnp.where(row > 0, under, border[y]) - flux_z)
            )
            border[y] = under
            return flux_y

        _, bottom = flux(volume[1, at, :] - volume[0, at, :], old[1, 0, at, :])
        inside = cells_y - 2
        steps = max(u for u in range(1, 8) if inside % u == 0)

        def several(k, before):
            for i in range(steps):
                y = 1 + k * steps + i
                before = plane(y, volume[y + 1, at, :], before, True)
            return before

        before = lax.fori_loop(0, inside // steps, several, bottom)
        for copy in halo_y(volume, slot, o):
            copy.wait()
        new, lower_y = flux(volume[0, at, :] - last_y[slot, at, :], low_by[at, :])
        if not first:
            low_by[at, :] = new
        plane(0, volume[1, at, :], jnp.where(iy > 0, lower_y, 0.0), True)
        plane(cells_y - 1, next_y[slot, at, :], before, iy < size_y - 1)

    def send_octet(o):
        block = split(src[o].reshape(rows, extent))
        spec[o] = product((xh[...], xl[...]), block, ((1,), (1,)))
        for d in others_y:
            forth(0, o, d).start()
        for h in range(HALVES):
            front[o, iy, inner(h), :] = spec[o, band(h, iy), :]

    def send_rest():
        for h in range(1, HALVES):
            for o in range(octets):
                for d in others_y:
                    forth(h, o, d).start()

    def forward(slot, h):
        level = jnp.zeros((piece, full_y), jnp.float32)
        first = level
        for o in range(octets):
            for d in others_y:
                forth(h, o, d).wait_recv()
            for r in range(piece // OCTET):
                at = pl.ds(h * piece + r * OCTET, OCTET)
                for t in range(groups):
                    planes = swap_groups([front[o, t * OCTET + i, at, :] for i in range(OCTET)])
                    for i in range(OCTET):
                        depth[h, o * OCTET + i, pl.ds(r * OCTET, OCTET), pl.ds(t * LANES, LANES)] = planes[i]
            values = split(depth[h, octet(o)].reshape(OCTET * piece, full_y))
            values = product(values, (yh[...], yl[...]), ((1,), (0,)))
            values = values.reshape(OCTET, piece, full_y)
            for i in range(OCTET):
                j = o * OCTET + i
                level = (values[i] + level) * gain[j, inner(h), :]
                first = level if j == 0 else first + tail[j - 1, inner(h), :] * level
                depth[h, j] = level
        ends[slot, h, 0] = first
        ends[slot, h, 1] = level
        gathered[slot, iz, h, 0] = first
        gathered[slot, iz, h, 1] = level
        for d in others_z:
            around(slot, h, d).start()

    def backward(slot, h):
        for d in others_z:
            around(slot, h, d).wait_recv()
        left = jnp.zeros((piece, full_y), jnp.float32)
        right = left
        for q in range(size_z - 1):
            mirror = size_z - 1 - q
            here = gathered[slot, q, h, 1]
            there = gathered[slot, mirror, h, 0]
            if q > 0:
                near, far = chain[q, 0, inner(h), :], chain[q, 1, inner(h), :]
                here = here + near * left + far * gathered[slot, q, h, 0]
                there = there + near * right + far * gathered[slot, mirror, h, 1]
            left = jnp.where(q < iz, here, left)
            right = jnp.where(q < size_z - 1 - iz, there, right)
        link = [home[i, inner(h), :] for i in range(9)]
        bottom = ends[slot, h, 0] + link[6] * left + link[8] * right
        top = ends[slot, h, 1] + link[8] * left + link[7] * right
        from_left = left + link[0] * (link[3] * bottom + link[5] * top)
        value = right + link[1] * (link[2] * top + link[4] * bottom)
        for o in reversed(range(octets)):
            for i in reversed(range(OCTET)):
                j = o * OCTET + i
                value = (
                    depth[h, j] + from_left * tail[j, inner(h), :] + gain[j, inner(h), :] * value
                )
                depth[h, j] = value
            values = split(depth[h, octet(o)].reshape(OCTET * piece, full_y))
            values = product(values, (th[...], tl[...]), ((1,), (0,)))
            depth[h, octet(o)] = values.reshape(OCTET, piece, full_y)
            for r in range(piece // OCTET):
                at = pl.ds(r * OCTET, OCTET)
                for t in range(groups):
                    planes = swap_groups(
                        [depth[h, o * OCTET + i, at, pl.ds(t * LANES, LANES)] for i in range(OCTET)]
                    )
                    for i in range(OCTET):
                        back[h, o, t * OCTET + i, at, :] = planes[i]
            for d in others_y:
                home_copy(h, o, d).start()
            arrive[o, band(h, iy), :] = back[h, o, iy]

    def assemble(slot, h):
        at = pl.ds(h * half, half)
        for o in reversed(range(octets)):
            for d in others_y:
                home_copy(h, o, d).wait_recv()
            values = product(split(arrive[o, at, :].T), (xh[at, :], xl[at, :]), ((1,), (0,)))
            values = values.reshape(cells_y, OCTET, extent)
            if h > 0:
                values = values + u_ref[:, octet(o), :]
            u_ref[:, octet(o), :] = values
            if h == HALVES - 1:
                halo_start(u_ref, slot + 1, o)

    coefficients()
    for o in range(octets):
        pointwise(f_ref, b_in, 0, True, o)
        send_octet(o)
    send_rest()

    def iteration(slot, carry):
        for h in range(HALVES):
            forward(slot, h)
        for h in range(HALVES):
            backward(slot, h)
        for h in range(HALVES):
            for o in range(octets):
                for d in others_y:
                    forth(h, o, d).wait_send()
        for h in range(HALVES):
            assemble(slot, h)
        for h in range(HALVES):
            for o in range(octets):
                for d in others_y:
                    home_copy(h, o, d).wait_send()
            for d in others_z:
                around(slot, h, d).wait_send()
        for o in range(octets):
            pointwise(u_ref, b_ref, slot + 1, False, o)

            @pl.when(slot < ITERS - 1)
            def _():
                send_octet(o)

        @pl.when(slot < ITERS - 1)
        def _():
            send_rest()

        return carry

    lax.fori_loop(0, ITERS, iteration, 0)


def per_device(size_y, size_z, observed, bregman):
    f = jnp.transpose(observed, (1, 2, 0))
    b = jnp.transpose(bregman, (0, 2, 3, 1))
    cells_y, cells_z, extent = f.shape
    full_y = cells_y * size_y
    part = extent // size_y
    octets = cells_z // OCTET
    groups = size_y // OCTET
    order = np.array(
        [
            (t * OCTET + i) * cells_y + y
            for t in range(groups)
            for y in range(cells_y)
            for i in range(OCTET)
        ]
    )
    matrix_y = cosine_matrix(full_y)[:, order]
    waves_x = np.broadcast_to(laplace_values(extent)[:, None], (extent, LANES))
    waves_y = np.broadcast_to(laplace_values(full_y)[None, :], (OCTET, full_y))
    constants = [
        *halves(cosine_matrix(extent)),
        *halves(matrix_y.T),
        *halves(matrix_y),
        waves_x.astype(np.float32),
        waves_y.astype(np.float32),
    ]
    slots = ITERS + 1
    piece = part // HALVES
    flags = pltpu.SemaphoreType.DMA
    real = lambda *shape: pltpu.VMEM(shape, jnp.float32)
    u, b = pl.pallas_call(
        functools.partial(kernel, size_y, size_z),
        out_shape=(
            jax.ShapeDtypeStruct(f.shape, jnp.float32),
            jax.ShapeDtypeStruct(b.shape, jnp.float32),
        ),
        in_specs=[pl.BlockSpec(memory_space=pltpu.VMEM)] * (2 + len(constants)),
        out_specs=(pl.BlockSpec(memory_space=pltpu.VMEM),) * 2,
        scratch_shapes=[
            real(octets, cells_y, OCTET, extent),
            real(octets, extent, LANES),
            real(octets, size_y, part, LANES),
            real(HALVES, cells_z, piece, full_y),
            real(cells_z, part, full_y),
            real(cells_z, part, full_y),
            real(HALVES, octets, size_y, piece, LANES),
            real(octets, extent, LANES),
            real(9, part, full_y),
            real(ITERS, HALVES, 2, piece, full_y),
            real(ITERS, size_z, HALVES, 2, piece, full_y),
            real(size_z, 2, part, full_y),
            real(cells_y, extent),
            real(cells_y, OCTET, extent),
            real(slots, cells_z, extent),
            real(slots, cells_z, extent),
            real(slots, cells_y, extent),
            real(slots, cells_y, extent),
            real(slots, 2, cells_y, extent),
            real(cells_z, extent),
            real(cells_y, extent),
            flags((HALVES, octets, size_y)),
            flags((HALVES, octets, size_y)),
            flags((HALVES, octets, size_y)),
            flags((HALVES, octets, size_y)),
            flags((ITERS, HALVES, size_z)),
            flags((ITERS, HALVES, size_z)),
            flags((slots, 2, octets)),
            flags((slots, 2, octets)),
            flags((slots, 4)),
            flags((slots, 4)),
        ],
        compiler_params=pltpu.CompilerParams(collective_id=0, has_side_effects=True),
    )(f, b, *[jnp.asarray(c) for c in constants])
    return jnp.transpose(u, (2, 0, 1)), jnp.transpose(b, (0, 3, 1, 2))


def solution(mesh):
    return jax.shard_map(
        functools.partial(per_device, mesh.shape["gy"], mesh.shape["gz"]),
        mesh=mesh,
        in_specs=(P(None, "gy", "gz"), P(None, None, "gy", "gz")),
        out_specs=(P(None, "gy", "gz"), P(None, None, "gy", "gz")),
        check_vma=False,
    )
```
